32 devices in a mesh: row: 8 (over y, x, core), col: 4 (over z).
Axes of the slice: x: 2, y: 2, z: 4, core: 2. Of those that a mesh axis runs over, the one named last changes fastest.
Arguments:
- schur: float32 [16384, 16384], P(None, ('row', 'col')), may hold values from -0.3 to 0.3
- basis: float32 [16384, 128], P('row'), may hold values from -1 to 1, as said below
- eigen: float32 [16384], P('row'), may hold values from -4 to -1
- schur_basis: bfloat16 [16384, 16384], P('col', 'row'), may hold values from -0.046875 to 0.046875
- rhs: bfloat16 [16384, 16384], P('col', 'row'), may hold values from -18 to 18, as said below
- inputs: bfloat16 [16384, 64], P('col'), may hold values from -6 to 6
Outputs:
- solution: float32 [16384, 128], P('row')
- feedback: float32 [64, 16384], P(None, 'col')
The draws below stay inside these ranges and needn't reach their ends.
Inputs may be any that keep to these rules, and one draw needn't show every extreme that they name: `basis`: every block of 128 consecutive rows, starting at a multiple of 128, is an orthogonal 128 x 128 matrix. `rhs`: symmetric.
All inputs are finite; a program needn't handle non-finite values.
Results may differ from the reference program's by a relative error of at most 0.005.
Values may be sent and summed in bfloat16 or wider, within the bound.
A program may use at most 192 MiB of HBM per device.

```python
import jax
import jax.numpy as jnp
from jax import lax

N = 16384
TILE = 128
M = 64
W_COLS = 128


def draw_schur(key, part):
    return jnp.clip(0.05 * jax.random.normal(key, (N, N), jnp.float32), -0.3, 0.3)


def draw_basis(key, part):
    raw = jax.random.normal(key, (N // TILE, TILE, TILE), jnp.float32)
    ortho, upper = jnp.linalg.qr(raw)
    return ortho.reshape(N, TILE)


def draw_rhs(key, part):
    raw = jnp.clip(jax.random.normal(key, (N, N), jnp.float32), -6.0, 6.0)
    sym = (raw + raw.T) * 0.7071
    return sym.astype(jnp.bfloat16)


def steps_of(stream_key, shape, cuts, smallest, high):
    def one(position, parts):
        draws = jax.random.uniform(jax.random.fold_in(jax.random.fold_in(stream_key, 6), position), (parts,), jnp.float32, smallest / len(cuts), high / len(cuts))
        return jnp.repeat(jnp.exp(draws), shape[position] // parts).reshape((-1,) + (1,) * (len(shape) - position - 1))

    level = one(*cuts[0])
    for cut in cuts[1:]:
        level = level * one(*cut)
    return level


def noise(rng, dims, deviation, bound, shards=(), held_as=jnp.bfloat16):
    result = deviation * jax.random.normal(rng, dims, jnp.float32)
    if shards:
        result = result * steps_of(rng, dims, shards, -0.22, 0.18)
    return jnp.clip(result, -bound, bound).astype(held_as)


def setup_inputs(seed: int = 0) -> dict:
    splits = jax.random.split(jax.random.key(seed), 7)
    schur = draw_schur(jax.random.fold_in(splits[6], 71), 0)
    basis = draw_basis(jax.random.fold_in(splits[6], 71), 0)
    eigen = jnp.clip(-4.0 + 3.0 * jax.random.uniform(splits[2], (N,), jnp.float32) ** steps_of(splits[2], (N,), ((0, 8),), -0.2, 0.2), -4.0, -1.0)
    schur_basis = noise(splits[3], (N, N), N ** -0.5, 0.046875, ((0, 4), (1, 8)))
    rhs = draw_rhs(jax.random.fold_in(splits[6], 71), 0)
    inputs = noise(splits[5], (N, M), 1.0, 6.0, ((0, 4),))
    return dict(schur=schur, basis=basis, eigen=eigen, schur_basis=schur_basis, rhs=rhs, inputs=inputs)


HIGH = lax.Precision.HIGHEST

def tile_solve(right, basis_left, eig_left, basis_right, eig_right):
    rotated = jnp.dot(jnp.dot(basis_left.T, right, precision=HIGH), basis_right, precision=HIGH)
    scaled = rotated / (eig_left[:, None] + eig_right[None, :])
    return jnp.dot(jnp.dot(basis_left, scaled, precision=HIGH), basis_right.T, precision=HIGH)

def solve_rows(right, panel, basis_rows, eig_rows, corner, corner_basis, corner_eig):
    count = right.shape[0] // TILE
    blocks = right.shape[1] // TILE

    def step(index, solved):
        start = index * TILE
        column = lax.dynamic_slice_in_dim(panel, start, TILE, 1)
        local = lax.dynamic_slice_in_dim(right, start, TILE, 0) - jnp.dot(column.T, solved, precision=HIGH)
        bas = lax.dynamic_slice_in_dim(basis_rows, start, TILE, 0)
        eig = lax.dynamic_slice_in_dim(eig_rows, start, TILE, 0)
        pieces = []
        for block in range(blocks):
            term = local[:, block * TILE:(block + 1) * TILE]
            for earlier in range(block):
                coupling = corner[earlier * TILE:(earlier + 1) * TILE, block * TILE:(block + 1) * TILE]
                term = term - jnp.dot(pieces[earlier], coupling, precision=HIGH)
            pieces.append(tile_solve(term, bas, eig, corner_basis[block * TILE:(block + 1) * TILE], corner_eig[block * TILE:(block + 1) * TILE]))
        return lax.dynamic_update_slice_in_dim(solved, jnp.concatenate(pieces, 1), start, 0)
    return lax.fori_loop(0, count, step, jnp.zeros(right.shape, jnp.float32))

def reference(schur, basis, eigen, schur_basis, rhs, inputs):
    window = schur_basis[:, :W_COLS]
    projected = jnp.dot(rhs.astype(jnp.float32), window.astype(jnp.float32), preferred_element_type=jnp.float32).astype(jnp.bfloat16)
    transformed = jnp.dot(schur_basis.T.astype(jnp.float32), projected.astype(jnp.float32), preferred_element_type=jnp.float32)
    solution = solve_rows(-transformed, schur, basis, eigen, schur[:W_COLS, :W_COLS], basis[:W_COLS], eigen[:W_COLS])
    reduced = jnp.dot(inputs.T.astype(jnp.float32), schur_basis.astype(jnp.float32), preferred_element_type=jnp.float32)
    gain = jnp.dot(reduced, solution, precision=HIGH)
    feedback = jnp.dot(gain, window.astype(jnp.float32).T, precision=HIGH)
    return (solution, feedback)
```

```python
import functools

import jax
import jax.numpy as jnp
from jax import lax
from jax.experimental import pallas as pl
from jax.experimental.pallas import tpu as pltpu
from jax.sharding import PartitionSpec as P

TILE = 128
W_COLS = 128


HIGH = lax.Precision.HIGHEST


def spread(x, axis, root):
    mine = lax.axis_index(axis) == root
    return lax.psum(jnp.where(mine, x, jnp.zeros_like(x)), axis)


def solve_kernel(groups, where_ref, panel_ref, turn_ref, basis_ref, scale_ref, *refs):
    pieces = refs[:groups]
    out_ref, rounded_ref, right, solved = refs[groups:]
    mine = where_ref[0]
    tiles = pieces[0].shape[0] // TILE
    count = out_ref.shape[0] // TILE
    for distance in range(groups):
        base = lax.rem(mine - distance + groups, groups) * tiles
        for tile in range(tiles):
            start = pl.multiple_of((base + tile) * TILE, TILE)
            right[pl.ds(start, TILE), :] = jnp.dot(
                turn_ref[base + tile],
                pieces[distance][tile * TILE : (tile + 1) * TILE, :],
                precision=HIGH,
                preferred_element_type=jnp.float32,
            )
    solved[...] = jnp.zeros_like(solved)

    def step(index, carry):
        start = pl.multiple_of(index * TILE, TILE)
        rows = pl.ds(start, TILE)
        both = jnp.dot(panel_ref[rows, :], solved[...], preferred_element_type=jnp.float32)
        value = right[rows, :] - (both[:, :W_COLS] + both[:, W_COLS:])
        value = value * scale_ref[rows, :]
        high = value.astype(jnp.bfloat16)
        low = (value - high.astype(jnp.float32)).astype(jnp.bfloat16)
        solved[rows, :W_COLS] = high
        solved[rows, W_COLS:] = low
        right[rows, :] = value
        return carry

    lax.fori_loop(0, count, step, 0)
    for tile in range(count):
        rows = slice(tile * TILE, (tile + 1) * TILE)
        back = jnp.dot(
            basis_ref[tile], right[rows, :], precision=HIGH, preferred_element_type=jnp.float32
        )
        out_ref[rows, :] = back
        rounded_ref[rows, :] = back.astype(jnp.bfloat16)


def solve_rows(where, panel, turn, basis, scale, pieces):
    span = panel.shape[0]
    vmem = pl.BlockSpec(memory_space=pltpu.VMEM)
    groups = len(pieces)
    return pl.pallas_call(
        functools.partial(solve_kernel, groups),
        out_shape=(
            jax.ShapeDtypeStruct((span, W_COLS), jnp.float32),
            jax.ShapeDtypeStruct((span, W_COLS), jnp.bfloat16),
        ),
        in_specs=[pl.BlockSpec(memory_space=pltpu.SMEM)] + [vmem] * (4 + groups),
        out_specs=(vmem, vmem),
        scratch_shapes=[
            pltpu.VMEM((span, W_COLS), jnp.float32),
            pltpu.VMEM((span, 2 * W_COLS), jnp.bfloat16),
        ],
        compiler_params=pltpu.CompilerParams(vmem_limit_bytes=32 * 1024 * 1024),
        cost_estimate=pl.CostEstimate(
            flops=4 * span * span * W_COLS, bytes_accessed=32 * span * TILE * 16, transcendentals=0
        ),
    )(where, panel, turn, basis, scale, *pieces)


def on_device(schur, basis, eigen, schur_basis, rhs, inputs):
    span = schur_basis.shape[1]
    width = schur.shape[1]
    chain = lax.axis_size("row")
    groups = lax.axis_size("col")
    ratio = chain // groups
    row_index = lax.axis_index("row")
    col_index = lax.axis_index("col")
    vectors = basis.reshape(span // TILE, TILE, TILE)
    turn = vectors.transpose(0, 2, 1)

    corner = spread(jnp.concatenate([basis[:W_COLS], eigen[None, :W_COLS]], 0), "row", 0)
    corner_basis, corner_eig = corner[:W_COLS], corner[W_COLS]

    panel_rows = lax.dynamic_slice_in_dim(schur, row_index * span, span, 0)
    own = lax.dynamic_slice_in_dim(vectors, col_index * (width // TILE), width // TILE, 0)
    blocks = panel_rows.reshape(span // TILE, TILE, width)
    left = jnp.einsum("tik,tic->tkc", vectors, blocks, precision=lax.Precision.HIGH)
    left = left.reshape(span, width // TILE, TILE)
    rotated = jnp.einsum("rtj,tjl->tlr", left, own, precision=lax.Precision.HIGH)
    panel = lax.all_gather(
        rotated.reshape(width, span).astype(jnp.bfloat16), "col", axis=0, tiled=True
    )
    scale = 1.0 / (eigen[:, None] + corner_eig[None, :])

    window = spread(schur_basis[:, :W_COLS], "row", 0)
    offset = row_index % ratio * span
    mine = lax.dynamic_slice_in_dim(window, offset, span, 0)
    own_window = spread(mine, "col", row_index // ratio)
    partial_value = jnp.dot(rhs, own_window, preferred_element_type=jnp.float32)
    projected = lax.psum(partial_value, "row").astype(jnp.bfloat16)
    coords = lax.dot_general(
        schur_basis, projected, (((0,), (0,)), ((), ())), preferred_element_type=jnp.float32
    )
    share = lax.psum_scatter(coords, "col", scatter_dimension=0, tiled=True)
    residual = -jnp.dot(share, corner_basis, precision=HIGH)
    where = col_index.astype(jnp.int32)[None]
    mapped = lax.dot_general(
        inputs, schur_basis, (((0,), (0,)), ((), ())), preferred_element_type=jnp.float32
    )

    def update(index, block):
        return lax.dot_general(
            schur[index * span : (index + 1) * span],
            block.astype(jnp.float32),
            (((0,), (0,)), ((), ())),
            precision=lax.Precision.HIGH,
            preferred_element_type=jnp.float32,
        )

    solution = jnp.zeros((span, W_COLS), jnp.float32)
    for index in range(chain):
        pieces = [residual] + [
            lax.ppermute(residual, "col", [(g, (g + d) % groups) for g in range(groups)])
            for d in range(1, groups)
        ]
        solved, rounded = solve_rows(where, panel, turn, vectors, scale, pieces)
        solution = jnp.where(row_index == index, solved, solution)
        if index + 1 < chain:
            block = lax.ppermute(rounded, "row", [(index, index + 1)])
            near = update(index, block)
        if index > 0 and index + 1 < chain:
            residual = residual - far
        if index + 1 < chain:
            residual = residual - near
        if index + 2 < chain:
            blocks = [lax.ppermute(rounded, "row", [(index, r)]) for r in range(index + 2, chain)]
            far = update(index, functools.reduce(jnp.add, blocks))
        else:
            far = jnp.zeros_like(residual)
    solution = jnp.dot(solution, corner_basis.T, precision=HIGH)
    gain = lax.psum(jnp.dot(mapped, solution, precision=HIGH), ("row", "col"))
    feedback = jnp.dot(gain, window.astype(jnp.float32).T, precision=HIGH)
    return (solution, feedback)


def solution(mesh):
    placed = (
        P(None, ("row", "col")),
        P("row", None),
        P("row"),
        P("col", "row"),
        P("col", "row"),
        P("col", None),
    )
    return jax.shard_map(
        on_device,
        mesh=mesh,
        in_specs=placed,
        out_specs=(P("row", None), P(None, "col")),
        check_vma=False,
    )
```
